32 devices in a mesh: mb: 4 (over z), tp: 2 (over y), dp: 4 (over x, core).
Axes of the slice: x: 2, y: 2, z: 4, core: 2. Of those that a mesh axis runs over, the one named last changes fastest.
Arguments:
- hidden: bfloat16 [4, 8, 512, 7168], P('dp', 'mb', None, 'tp'), may hold values from -6 to 6
- latent: bfloat16 [4, 8, 512, 512], P('dp', 'mb', None, 'tp'), may hold values from -6 to 6
- out_grad: bfloat16 [4, 8, 512, 16384], P('dp', 'mb', None, 'tp'), may hold values from -0.059814453 to 0.059814453
- up_weight: bfloat16 [512, 16384], P(None, 'tp'), may hold values from -0.046875 to 0.046875
- mb_tokens: int32 [4, 8], P('dp'), may hold values from 128 to 512, as said below
- slot_mb: int32 [4, 8], P('dp', 'mb'), may hold values from 0 to 7, each once within a row
Outputs:
- up_grad: float32 [512, 16384], P(('mb', 'dp'), 'tp')
- running_down: float32 [4, 7168, 512], P('mb', 'tp', 'dp')
The draws below stay inside these ranges and needn't reach their ends.
Inputs may be any that keep to these rules, and one draw needn't show every extreme that they name: `mb_tokens`: each count is a multiple of 128; in every group some microbatch has exactly 512 tokens. `slot_mb`: each row is a permutation of the microbatch numbers.
All inputs are finite; a program needn't handle non-finite values.
Results may differ from the reference program's by a relative error of at most 0.005.
Values may be sent and summed in bfloat16 or wider, within the bound.
A program may use at most 128 MiB of HBM per device.

```python
import jax
import jax.numpy as jnp
from jax import lax

D = 7168
R = 512
COLS = 16384
TOKBLOCK = 128
CAP = 512
SLOTS = 2
MICRO = 8
GROUPS = 4
N_MB = 4


def draw_mb_tokens(key, part):
    first_key, second_key = jax.random.split(jax.random.fold_in(key, 11))
    blocks = jax.random.randint(first_key, (GROUPS, MICRO), 1, CAP // TOKBLOCK + 1)
    chosen = jax.random.randint(second_key, (GROUPS, 1), 0, MICRO)
    blocks = jnp.where(jnp.arange(MICRO)[None, :] == chosen, CAP // TOKBLOCK, blocks)
    return (blocks * TOKBLOCK).astype(jnp.int32)


def block_scale(own_key, dims, cuts, smallest, top_value):
    level, own = 1.0, jax.random.fold_in(own_key, 6)
    for axis_at, shards_of in cuts:
        steps = jnp.exp(jax.random.uniform(jax.random.fold_in(own, axis_at), (shards_of,), jnp.float32, smallest / len(cuts), top_value / len(cuts)))
        level = level * jnp.repeat(steps, dims[axis_at] // shards_of).reshape([-1 if axis == axis_at else 1 for axis in range(len(dims))])
    return level


def noise(rng, shape, scale, limit, cuts=(), kind=jnp.bfloat16):
    values = jax.random.normal(rng, shape, jnp.float32) * scale
    if len(cuts) > 0:
        values = block_scale(rng, shape, cuts, -0.22, 0.18) * values
    return jnp.clip(values, min=-limit, max=limit).astype(kind)


def setup_inputs(seed: int = 0) -> dict:
    key_of = jax.random.split(jax.random.key(seed), 7)
    return {
        "hidden": noise(key_of[0], (GROUPS, MICRO, CAP, D), 1.0, 6.0, ((0, 4), (1, 4), (3, 2))),
        "latent": noise(key_of[1], (GROUPS, MICRO, CAP, R), 1.0, 6.0, ((0, 4), (1, 4), (3, 2))),
        "out_grad": noise(key_of[2], (GROUPS, MICRO, CAP, COLS), 0.01, 0.059814453, ((0, 4), (1, 4), (3, 2))),
        "up_weight": noise(key_of[3], (R, COLS), COLS ** -0.5, 0.046875, ((1, 2),)),
        "mb_tokens": draw_mb_tokens(jax.random.fold_in(key_of[6], 71), 0),
        "slot_mb": jax.vmap(lambda own: jax.random.permutation(own, MICRO))(jax.random.split(key_of[5], GROUPS)).reshape((GROUPS, MICRO)).astype(jnp.int32),
    }


def reference(hidden, latent, out_grad, up_weight, mb_tokens, slot_mb):
    counts = jnp.take_along_axis(mb_tokens, slot_mb, axis=1).reshape(-1)
    owners = jnp.tile(jnp.arange(MICRO, dtype=jnp.int32) // SLOTS, GROUPS)
    positions = jnp.arange(CAP, dtype=jnp.int32)

    def accumulate(carry, inputs_now):
        up_total, down_owner = carry
        hidden_rows, latent_rows, grad_rows, length, owner_id = inputs_now
        masked = jnp.where((positions < length)[:, None], grad_rows, jnp.zeros((), grad_rows.dtype))
        latent_grad = jnp.dot(masked, up_weight.T, preferred_element_type=jnp.float32).astype(jnp.bfloat16)
        up_total = up_total + jnp.dot(latent_rows.T, masked, preferred_element_type=jnp.float32)
        down_term = jnp.dot(hidden_rows.T, latent_grad, preferred_element_type=jnp.float32)
        down_owner = down_owner.at[owner_id].add(down_term)
        return (up_total, down_owner), None

    start_state = (jnp.zeros((R, COLS), jnp.float32), jnp.zeros((N_MB, D, R), jnp.float32))
    sequence = (hidden.reshape(-1, CAP, D), latent.reshape(-1, CAP, R), out_grad.reshape(-1, CAP, COLS), counts, owners)
    (up_total, down_owner), unused = lax.scan(accumulate, start_state, sequence)
    return up_total, jnp.cumsum(down_owner, axis=0)
```

```python
import functools

import jax
import jax.numpy as jnp
from jax import lax
from jax.experimental import pallas as pl
from jax.experimental.pallas import tpu as pltpu
from jax.sharding import PartitionSpec as P

F32 = jnp.float32
BF16 = jnp.bfloat16
UP_CHUNKS = 8
LATE = 1
LAG = 4
TRAIL = 3


def bits_of(size):
    count = size.bit_length() - 1
    assert size == 1 << count, "axis size"
    return count


def kernel(sizes, hidden, latent, grad, weight, tokens, slots, up_out, run_out,
           grad_v, weight_v, hidden_v, lat_v, lat_t, lg_acc, lg_send, lg_recv, lg_t,
           up, up_r, dn, dn_r, pre_r,
           grad_sem, weight_sem, hidden_sem, lat_sem, lat_ss, lat_rs, lg_ss, lg_rs,
           up_ss, up_rs, dn_ss, dn_rs, pre_ss, pre_rs):
    n_mb, n_tp, n_dp = sizes
    mb, tp, dp = (lax.axis_index(a) for a in ("mb", "tp", "dp"))
    up_chunks, slot_count, cap, width = grad_v.shape
    rows = slot_count * cap
    rank_part = lat_v.shape[-1]
    down_chunks, down_width = dn.shape[0], dn.shape[-1]
    ahead = hidden_v.shape[0]

    dims, partner = [], {}
    for axis, index, size in (("mb", mb, n_mb), ("dp", dp, n_dp)):
        for k in reversed(range(bits_of(size))):
            bit = (index // (1 << k)) % 2
            dims.append((axis, k))
            partner[axis, k] = bit, {axis: index + (1 - 2 * bit) * (1 << k)}
    tp_bits, n_dp_steps = bits_of(n_tp), bits_of(n_dp)
    part_dims = dims[:tp_bits]
    last = len(dims) - 1
    dp_first = dims[::-1]
    mb_first = dp_first[:1] + dp_first[n_dp_steps:] + dp_first[1:n_dp_steps]
    orders = (dp_first, mb_first)
    joints = [min(order.index(d) for d in part_dims) if part_dims else last for order in orders]
    tp_peers = [{"tp": (tp + s) % n_tp} for s in range(1, n_tp)]
    following, preceding = {"mb": (mb + 1) % n_mb}, {"mb": (mb + n_mb - 1) % n_mb}

    def grad_copy(c):
        return pltpu.make_async_copy(
            grad.at[0, :, :, pl.ds(pl.multiple_of(c * width, width), width)], grad_v.at[c], grad_sem.at[c])

    def weight_copy(c):
        return pltpu.make_async_copy(
            weight.at[:, pl.ds(pl.multiple_of(c * width, width), width)], weight_v.at[c], weight_sem.at[c])

    def hidden_copy(c):
        return pltpu.make_async_copy(
            hidden.at[0, :, :, pl.ds(pl.multiple_of(c * down_width, down_width), down_width)],
            hidden_v.at[c % ahead], hidden_sem.at[c % ahead])

    def remote(src, dst, ss, rs, to):
        return pltpu.make_async_remote_copy(
            src_ref=src, dst_ref=dst, send_sem=ss, recv_sem=rs,
            device_id=to, device_id_type=pl.DeviceIdType.MESH)

    barrier = pltpu.get_barrier_semaphore()
    greeted = [to for _, to in partner.values()] + tp_peers + [following, preceding]
    for to in greeted:
        pl.semaphore_signal(barrier, inc=1, device_id=to, device_id_type=pl.DeviceIdType.MESH)

    own_latent = pltpu.make_async_copy(latent.at[0], lat_v.at[0], lat_sem)
    own_latent.start()
    first = up_chunks - LATE
    late = range(first, up_chunks)
    fetched = [c for i in range(LATE) for c in (i, first + i)] + list(range(LATE, first))
    grad_copy(fetched[0]).start()

    counts = [tokens[0, slots[0, s]] for s in range(slot_count)]

    def live(shape):
        row = lax.broadcasted_iota(jnp.int32, shape, 0)
        valid = row < counts[0]
        for s in range(1, slot_count):
            valid = valid | ((row >= s * cap) & (row < s * cap + counts[s]))
        return valid

    def latent_part(s):
        part = lat_v[s].reshape(rows, rank_part).astype(F32)
        part = jnp.where(live(part.shape), part, 0.0)
        lat_t[s] = part.T.astype(BF16)

    own_latent.wait()
    for c in fetched[1:3]:
        grad_copy(c).start()
    latent_part(0)
    pl.semaphore_wait(barrier, len(greeted))

    def lat_copy(s):
        return remote(lat_v.at[0], lat_v.at[s], lat_ss.at[s - 1], lat_rs.at[s - 1], tp_peers[s - 1])

    def lg_copy(s, slot):
        return remote(lg_send.at[slot], lg_recv.at[s - 1, slot],
                      lg_ss.at[s - 1, slot], lg_rs.at[s - 1, slot], tp_peers[s - 1])

    for s in range(1, n_tp):
        lat_copy(s).start()
    for c in fetched[3:]:
        grad_copy(c).start()
    for c in range(up_chunks):
        weight_copy(c).start()
    for c in range(ahead):
        hidden_copy(c).start()

    def part_at(s):
        part = (tp + n_tp - s) % n_tp
        return {d: (part // (1 << k)) % 2 for k, d in enumerate(reversed(part_dims))}

    def up_refs(o, k, s, c, side):
        step = orders[o][k]
        bit, to = partner[step]
        fixed = part_at(s) if k < joints[o] else {}
        taken = {**fixed, step: (1 - bit) if side else bit}
        before = [d for d in dims if d not in orders[o][:k]]
        after = [d for d in before if d != step]
        src = (up if k == 0 else up_r[k - 1], (c,) + tuple(taken.get(d, slice(None)) for d in before))
        dst = (up_r[k], (c,) + tuple(fixed.get(d, slice(None)) for d in after))
        return src, dst, to

    def up_copy(o, k, s, c):
        (src, at), (dst, to_at), to = up_refs(o, k, s, c, 1)
        return remote(src.at[at], dst.at[to_at], up_ss.at[k, s, c], up_rs.at[k, s, c], to)

    def up_add(o, k, s, c):
        (src, at), (dst, to_at), _ = up_refs(o, k, s, c, 0)
        up_copy(o, k, s, c).wait_recv()
        return src[at].astype(F32) + dst[to_at].astype(F32)

    def up_pass(o, k, s, c):
        _, (dst, to_at), _ = up_refs(o, k, s, c, 0)
        dst[to_at] = up_add(o, k, s, c).astype(BF16)
        if k + 1 != joints[o]:
            up_copy(o, k + 1, s, c).start()

    def up_make(s, c):
        block = lax.dot_general(
            lat_t[s], grad_v[c].reshape(rows, width),
            (((1,), (0,)), ((), ())), preferred_element_type=F32).astype(BF16)
        fixed = part_at(s)
        head = tuple(fixed[d] for d in part_dims)
        up[(c,) + head] = block.reshape(up.shape[1 + tp_bits:])
        up_copy(0, 0, s, c).start()

    def up_deep(o, s, c, k):
        for j in range(k, joints[o]):
            up_pass(o, j, s, c)

    def up_finish(o, c):
        for j in range(joints[o], last):
            up_pass(o, j, 0, c)
        up_write(o, c)

    def up_write(o, c):
        at = pl.ds(pl.multiple_of(c * width, width), width)
        up_out[:, at] = up_add(o, last, 0, c)

    others = range(1, n_tp)

    def up_second(c):
        for s in others:
            up_pass(0, 1, s, c)

    def up_join(c):
        for s in others:
            up_deep(0, s, c, 2)
        up_copy(0, joints[0], 0, c).start()

    def dn_copy(k, c):
        bit, to = partner["dp", k]
        src = (dn if k == 0 else dn_r[k - 1]).at[c]
        index = (slice(None),) * (n_dp_steps - 1 - k) + (1 - bit,)
        return remote(src.at[index], dn_r[k].at[c], dn_ss.at[k, c], dn_rs.at[k, c], to)

    def dn_add(k, c):
        bit, _ = partner["dp", k]
        dn_copy(k, c).wait_recv()
        src = dn if k == 0 else dn_r[k - 1]
        kept = src[(c,) + (slice(None),) * (n_dp_steps - 1 - k) + (bit,)]
        return kept.astype(F32) + dn_r[k][c].astype(F32)

    def dn_pass(k, c):
        dn_r[k][c] = dn_add(k, c).astype(BF16)
        dn_copy(k + 1, c).start()

    def pre_copy(c):
        return remote(dn.at[pre_at(c)], pre_r.at[c], pre_ss.at[c], pre_rs.at[c], following)

    def pre_at(c):
        return (c,) + (0,) * (n_dp_steps - 1) + (partner["dp", 0][0],)

    def run_at(c):
        return pl.ds(pl.multiple_of(c * down_width, down_width), down_width)

    def dn_share(c):
        for k in range(1, n_dp_steps - 1):
            dn_pass(k, c)
        share = dn_add(n_dp_steps - 1, c)

        run_out[0, run_at(c), :] = share.T

        @pl.when(mb == 0)
        def _():
            dn[pre_at(c)] = share.astype(BF16)
            pre_copy(c).start()

    def prefix(c):
        @pl.when((mb > 0) & (c >= 0) & (c < down_chunks))
        def _():
            pre_copy(c).wait_recv()
            running = run_out[0, run_at(c), :] + pre_r[c].astype(F32).T
            run_out[0, run_at(c), :] = running

            @pl.when(mb < n_mb - 1)
            def _():
                dn[pre_at(c)] = running.T.astype(BF16)
                pre_copy(c).start()

    def lg_step(slot, j):
        total = lg_acc[slot]
        for c in (2 * j, 2 * j + 1):
            total = total + lax.dot_general(
                weight_v[c], grad_v[c, slot], (((1,), (1,)), ((), ())), preferred_element_type=F32)
        lg_acc[slot] = total

    def lg_start(slot):
        lg_send[slot] = lg_acc[slot].astype(BF16)
        for s in others:
            lg_copy(s, slot).start()

    pairs = up_chunks // 2
    lg_acc[...] = jnp.zeros_like(lg_acc)

    @pl.loop(0, LATE)
    def _(i):
        for c in (i, first + i):
            grad_copy(c).wait()
            up_make(0, c)

        @pl.when(i >= 1)
        def _():
            up_pass(0, 0, 0, i - 1)
            up_pass(1, 0, 0, first + i - 1)

    @pl.loop(LATE, first)
    def _(c):
        grad_copy(c).wait()
        up_make(0, c)

        @pl.when(c == LATE)
        def _():
            up_pass(0, 0, 0, LATE - 1)

        @pl.when(c == LATE + 1)
        def _():
            up_pass(1, 0, 0, up_chunks - 1)

        @pl.when(c >= LATE + 2)
        def _():
            up_pass(0, 0, 0, c - 2)

    @pl.loop(0, pairs)
    def _(j):
        for c in (2 * j, 2 * j + 1):
            weight_copy(c).wait()
        lg_step(0, j)

        @pl.when(j < 2)
        def _():
            up_pass(0, 0, 0, first - 2 + j)

        @pl.when(j % 2 == 1)
        def _():
            up_pass(0, 1, 0, j // 2)

    lg_start(0)

    for s in others:
        lat_copy(s).wait_recv()
        latent_part(s)
        for c in late:
            up_make(s, c)

    for slot in range(1, slot_count):
        @pl.loop(0, pairs)
        def _(j):
            lg_step(slot, j)
            if slot == 1:
                @pl.when(j == 0)
                def _():
                    for s in others:
                        for c in late:
                            up_pass(1, 0, s, c)
                    up_pass(0, 1, 0, 2)

                @pl.when(j % 2 == 1)
                def _():
                    up_deep(0, 0, j // 2, 2)

        lg_start(slot)
    up_pass(0, 1, 0, 3)

    for s in others:
        @pl.loop(0, first)
        def _(c):
            up_make(s, c)

            @pl.when(c >= 2)
            def _():
                up_pass(0, 0, s, c - 2)

            if s == 1:
                @pl.when((c == 2) | (c == 6))
                def _():
                    up_pass(0, 1, 0, 4 + c // 4)

        for c in range(first - 2, first):
            up_pass(0, 0, s, c)

    up_deep(0, 0, 2, 2)
    up_deep(0, 0, 3, 2)
    for c in range(6, first):
        up_pass(0, 1, 0, c)
    for c in late:
        for s in range(n_tp):
            up_deep(1, s, c, 1)
        up_copy(1, joints[1], 0, c).start()
    up_deep(0, 0, 4, 2)
    up_second(0)
    up_deep(0, 0, 5, 2)
    up_second(1)
    for c in range(6, first):
        up_deep(0, 0, c, 2)
    up_join(0)
    up_second(2)
    up_join(1)

    for slot in range(slot_count):
        total = lg_acc[slot]
        for s in others:
            lg_copy(s, slot).wait_recv()
            total = total + lg_recv[s - 1, slot].astype(F32)
        token = lax.broadcasted_iota(jnp.int32, total.shape, 1)
        total = jnp.where(token < counts[slot], total, 0.0)
        lg_t[:, slot * cap:(slot + 1) * cap] = total.astype(BF16)

    @pl.loop(0, down_chunks)
    def _(c):
        hidden_copy(c).wait()
        block = lax.dot_general(
            lg_t[...], hidden_v[c % ahead].reshape(rows, down_width),
            (((1,), (0,)), ((), ())), preferred_element_type=F32)
        dn[c] = block.astype(BF16).reshape(dn.shape[1:])
        dn_copy(0, c).start()

        @pl.when(c + ahead < down_chunks)
        def _():
            hidden_copy(c + ahead).start()

        @pl.when(c >= TRAIL)
        def _():
            dn_pass(0, c - TRAIL)

        for n, at in enumerate((2, 4, 6)):
            @pl.when(c == down_chunks * at // 7)
            def _():
                up_second(3 + n)
                up_join(2 + n)

    for c in range(down_chunks - TRAIL, down_chunks):
        dn_pass(0, c)
    for c in late:
        up_pass(1, joints[1], 0, c)
    for c in range(6, first):
        up_second(c)
        up_join(c - 1)

    @pl.loop(0, down_chunks)
    def _(t):
        dn_share(t)

        @pl.when(t == 2)
        def _():
            up_join(first - 1)

        prefix(t - LAG * mb)

    @pl.loop(0, first)
    def _(c):
        up_finish(0, c)

    for c in late:
        for j in range(joints[1] + 1, last):
            up_pass(1, j, 0, c)
        up_write(1, c)

    @pl.loop(0, LAG * (n_mb - 1))
    def _(u):
        prefix(down_chunks + u - LAG * mb)

    for s in others:
        lat_copy(s).wait_send()
        for slot in range(slot_count):
            lg_copy(s, slot).wait_send()

    def up_sent(o, c):
        for k in range(last + 1):
            for s in range(n_tp if k < joints[o] else 1):
                up_copy(o, k, s, c).wait_send()

    @pl.loop(0, first)
    def _(c):
        up_sent(0, c)

    for c in late:
        up_sent(1, c)

    @pl.loop(0, down_chunks)
    def _(c):
        for k in range(n_dp_steps):
            dn_copy(k, c).wait_send()

        @pl.when(mb < n_mb - 1)
        def _():
            pre_copy(c).wait_send()


def local(sizes, hidden, latent, out_grad, up_weight, mb_tokens, slot_mb):
    n_mb, n_tp, n_dp = sizes
    _, slot_count, cap, feature_part = hidden.shape
    rank_part = latent.shape[3]
    rank, column_part = up_weight.shape
    rows = slot_count * cap
    width = column_part // UP_CHUNKS
    down_chunks = next(n for n in (14, 7) if feature_part % (128 * n) == 0)
    down_width = feature_part // down_chunks
    ahead = 2 * down_chunks // 7
    dp_bits, mb_bits = bits_of(n_dp), bits_of(n_mb)
    bits = dp_bits + mb_bits
    up_rows = rank >> bits
    share = rank >> dp_bits
    dma = pltpu.SemaphoreType.DMA
    scratch = [
        pltpu.VMEM((UP_CHUNKS, slot_count, cap, width), BF16),
        pltpu.VMEM((UP_CHUNKS, rank, width), BF16),
        pltpu.VMEM((ahead, slot_count, cap, down_width), BF16),
        pltpu.VMEM((n_tp, slot_count, cap, rank_part), BF16),
        pltpu.VMEM((n_tp, rank_part, rows), BF16),
        pltpu.VMEM((slot_count, rank, cap), F32),
        pltpu.VMEM((slot_count, rank, cap), BF16),
        pltpu.VMEM((n_tp - 1, slot_count, rank, cap), BF16),
        pltpu.VMEM((rank, rows), BF16),
        pltpu.VMEM((UP_CHUNKS,) + (2,) * bits + (up_rows, width), BF16),
        [pltpu.VMEM((UP_CHUNKS,) + (2,) * (bits - 1 - k) + (up_rows, width), BF16) for k in range(bits)],
        pltpu.VMEM((down_chunks,) + (2,) * dp_bits + (share, down_width), BF16),
        [pltpu.VMEM((down_chunks,) + (2,) * (dp_bits - 1 - k) + (share, down_width), BF16) for k in range(dp_bits)],
        pltpu.VMEM((down_chunks, share, down_width), BF16),
        dma((UP_CHUNKS,)), dma((UP_CHUNKS,)), dma((ahead,)), dma,
        dma((n_tp - 1,)), dma((n_tp - 1,)), dma((n_tp - 1, slot_count)), dma((n_tp - 1, slot_count)),
        dma((bits, n_tp, UP_CHUNKS)), dma((bits, n_tp, UP_CHUNKS)),
        dma((dp_bits, down_chunks)), dma((dp_bits, down_chunks)),
        dma((down_chunks,)), dma((down_chunks,)),
    ]
    hbm = pl.BlockSpec(memory_space=pl.ANY)
    smem = pl.BlockSpec(memory_space=pltpu.SMEM)
    vmem = pl.BlockSpec(memory_space=pltpu.VMEM)
    return pl.pallas_call(
        functools.partial(kernel, sizes),
        out_shape=(
            jax.ShapeDtypeStruct((up_rows, column_part), F32),
            jax.ShapeDtypeStruct((1, feature_part, share), F32),
        ),
        in_specs=[hbm] * 4 + [smem] * 2,
        out_specs=(vmem, vmem),
        scratch_shapes=scratch,
        compiler_params=pltpu.CompilerParams(
            collective_id=0, has_side_effects=True, vmem_limit_bytes=67043328),
    )(hidden, latent, out_grad, up_weight, mb_tokens, slot_mb)


def solution(mesh):
    sizes = tuple(mesh.shape[axis] for axis in ("mb", "tp", "dp"))
    return jax.shard_map(
        functools.partial(local, sizes),
        mesh=mesh,
        in_specs=(
            P("dp", "mb", None, "tp"),
            P("dp", "mb", None, "tp"),
            P("dp", "mb", None, "tp"),
            P(None, "tp"),
            P("dp", None),
            P("dp", "mb"),
        ),
        out_specs=(P(("mb", "dp"), "tp"), P("mb", "tp", "dp")),
        check_vma=False,
    )
```

```python
import functools

import jax
import jax.numpy as jnp
from jax import lax
from jax.experimental import pallas as pl
from jax.experimental.pallas import tpu as pltpu
from jax.sharding import PartitionSpec as P

F32 = jnp.float32
BF16 = jnp.bfloat16
UP_CHUNKS = 8
LATE = 2
EARLY = 4
LAG = 4
TRAIL = 2


def bits_of(size):
    count = size.bit_length() - 1
    assert size == 1 << count, "axis size"
    return count


def kernel(sizes, hidden, latent, grad, weight, tokens, slots, up_out, run_out,
           grad_v, weight_v, hidden_v, lat_v, lat_t, lg_acc, lg_send, lg_recv, lg_t,
           up, up_r, dn, dn_r, pre_r,
           grad_sem, weight_sem, hidden_sem, lat_sem, lat_ss, lat_rs, lg_ss, lg_rs,
           up_ss, up_rs, dn_ss, dn_rs, pre_ss, pre_rs):
    n_mb, n_tp, n_dp = sizes
    mb, tp, dp = (lax.axis_index(a) for a in ("mb", "tp", "dp"))
    up_chunks, slot_count, cap, width = grad_v.shape
    rows = slot_count * cap
    rank_part = lat_v.shape[-1]
    down_chunks, down_width = dn.shape[0], dn.shape[-1]
    ahead = hidden_v.shape[0]

    dims, partner = [], {}
    for axis, index, size in (("mb", mb, n_mb), ("dp", dp, n_dp)):
        for k in reversed(range(bits_of(size))):
            bit = (index // (1 << k)) % 2
            dims.append((axis, k))
            partner[axis, k] = bit, {axis: index + (1 - 2 * bit) * (1 << k)}
    tp_bits, n_dp_steps = bits_of(n_tp), bits_of(n_dp)
    part_dims = dims[:tp_bits]
    last = len(dims) - 1
    dp_first = dims[::-1]
    mb_first = dp_first[:1] + dp_first[n_dp_steps:] + dp_first[1:n_dp_steps]
    orders = (dp_first, mb_first)
    joints = [min(order.index(d) for d in part_dims) if part_dims else last for order in orders]
    tp_peers = [{"tp": (tp + s) % n_tp} for s in range(1, n_tp)]
    following, preceding = {"mb": (mb + 1) % n_mb}, {"mb": (mb + n_mb - 1) % n_mb}

    def grad_copy(c):
        return pltpu.make_async_copy(
            grad.at[0, :, :, pl.ds(pl.multiple_of(c * width, width), width)], grad_v.at[c], grad_sem.at[c])

    def weight_copy(c):
        return pltpu.make_async_copy(
            weight.at[:, pl.ds(pl.multiple_of(c * width, width), width)], weight_v.at[c], weight_sem.at[c])

    def hidden_copy(c):
        return pltpu.make_async_copy(
            hidden.at[0, :, :, pl.ds(pl.multiple_of(c * down_width, down_width), down_width)],
            hidden_v.at[c % ahead], hidden_sem.at[c % ahead])

    def remote(src, dst, ss, rs, to):
        return pltpu.make_async_remote_copy(
            src_ref=src, dst_ref=dst, send_sem=ss, recv_sem=rs,
            device_id=to, device_id_type=pl.DeviceIdType.MESH)

    barrier = pltpu.get_barrier_semaphore()
    greeted = [to for _, to in partner.values()] + tp_peers + [following, preceding]
    for to in greeted:
        pl.semaphore_signal(barrier, inc=1, device_id=to, device_id_type=pl.DeviceIdType.MESH)

    own_latent = pltpu.make_async_copy(latent.at[0], lat_v.at[0], lat_sem)
    own_latent.start()
    first = up_chunks - LATE
    late = range(first, up_chunks)
    fetched = [0, late[0], 1, *late[1:], *range(2, first)]
    grad_copy(fetched[0]).start()

    counts = [tokens[0, slots[0, s]] for s in range(slot_count)]

    def live(shape):
        row = lax.broadcasted_iota(jnp.int32, shape, 0)
        valid = row < counts[0]
        for s in range(1, slot_count):
            valid = valid | ((row >= s * cap) & (row < s * cap + counts[s]))
        return valid

    def latent_part(s):
        part = lat_v[s].reshape(rows, rank_part).astype(F32)
        part = jnp.where(live(part.shape), part, 0.0)
        lat_t[s] = part.T.astype(BF16)

    own_latent.wait()
    for c in fetched[1:3]:
        grad_copy(c).start()
    latent_part(0)
    pl.semaphore_wait(barrier, len(greeted))

    def lat_copy(s):
        return remote(lat_v.at[0], lat_v.at[s], lat_ss.at[s - 1], lat_rs.at[s - 1], tp_peers[s - 1])

    def lg_copy(s, slot):
        return remote(lg_send.at[slot], lg_recv.at[s - 1, slot],
                      lg_ss.at[s - 1, slot], lg_rs.at[s - 1, slot], tp_peers[s - 1])

    for s in range(1, n_tp):
        lat_copy(s).start()
    for c in fetched[3:]:
        grad_copy(c).start()
    for c in range(up_chunks):
        weight_copy(c).start()
    for c in range(ahead):
        hidden_copy(c).start()

    def part_at(s):
        part = (tp + n_tp - s) % n_tp
        return {d: (part // (1 << k)) % 2 for k, d in enumerate(reversed(part_dims))}

    def up_refs(o, k, s, c, side):
        step = orders[o][k]
        bit, to = partner[step]
        fixed = part_at(s) if k < joints[o] else {}
        taken = {**fixed, step: (1 - bit) if side else bit}
        before = [d for d in dims if d not in orders[o][:k]]
        after = [d for d in before if d != step]
        src = (up if k == 0 else up_r[k - 1], (c,) + tuple(taken.get(d, slice(None)) for d in before))
        dst = (up_r[k], (c,) + tuple(fixed.get(d, slice(None)) for d in after))
        return src, dst, to

    def up_copy(o, k, s, c):
        (src, at), (dst, to_at), to = up_refs(o, k, s, c, 1)
        return remote(src.at[at], dst.at[to_at], up_ss.at[k, s, c], up_rs.at[k, s, c], to)

    def up_add(o, k, s, c, waited=False):
        (src, at), (dst, to_at), _ = up_refs(o, k, s, c, 0)
        if not waited:
            up_copy(o, k, s, c).wait_recv()
        return src[at].astype(F32) + dst[to_at].astype(F32)

    def up_pass(o, k, s, c, waited=False):
        _, (dst, to_at), _ = up_refs(o, k, s, c, 0)
        dst[to_at] = up_add(o, k, s, c, waited).astype(BF16)
        if k + 1 != joints[o]:
            up_copy(o, k + 1, s, c).start()

    def up_make(s, c):
        block = lax.dot_general(
            lat_t[s], grad_v[c].reshape(rows, width),
            (((1,), (0,)), ((), ())), preferred_element_type=F32).astype(BF16)
        fixed = part_at(s)
        head = tuple(fixed[d] for d in part_dims)
        up[(c,) + head] = block.reshape(up.shape[1 + tp_bits:])
        up_copy(0, 0, s, c).start()

    def up_deep(o, s, c, k):
        for j in range(k, joints[o]):
            up_pass(o, j, s, c)

    def up_finish(o, c, waited=False):
        for j in range(joints[o], last):
            up_pass(o, j, 0, c, waited and j == joints[o])
        up_write(o, c, waited and joints[o] == last)

    def up_write(o, c, waited=False):
        at = pl.ds(pl.multiple_of(c * width, width), width)
        up_out[:, at] = up_add(o, last, 0, c, waited)

    others = range(1, n_tp)

    def up_second(c):
        for s in others:
            up_pass(0, 1, s, c)

    def up_join(c):
        for s in others:
            up_deep(0, s, c, 2)
        up_copy(0, joints[0], 0, c).start()

    def dn_copy(k, c):
        bit, to = partner["dp", k]
        src = (dn if k == 0 else dn_r[k - 1]).at[c]
        index = (slice(None),) * (n_dp_steps - 1 - k) + (1 - bit,)
        return remote(src.at[index], dn_r[k].at[c], dn_ss.at[k, c], dn_rs.at[k, c], to)

    def dn_add(k, c):
        bit, _ = partner["dp", k]
        dn_copy(k, c).wait_recv()
        src = dn if k == 0 else dn_r[k - 1]
        kept = src[(c,) + (slice(None),) * (n_dp_steps - 1 - k) + (bit,)]
        return kept.astype(F32) + dn_r[k][c].astype(F32)

    def dn_pass(k, c):
        dn_r[k][c] = dn_add(k, c).astype(BF16)
        dn_copy(k + 1, c).start()

    def pre_copy(c):
        return remote(dn.at[pre_at(c)], pre_r.at[c], pre_ss.at[c], pre_rs.at[c], following)

    def pre_at(c):
        return (c,) + (0,) * (n_dp_steps - 1) + (partner["dp", 0][0],)

    def run_at(c):
        return pl.ds(pl.multiple_of(c * down_width, down_width), down_width)

    def dn_share(c):
        for k in range(1, n_dp_steps - 1):
            dn_pass(k, c)
        share = dn_add(n_dp_steps - 1, c)

        run_out[0, run_at(c), :] = share.T

        @pl.when(mb == 0)
        def _():
            dn[pre_at(c)] = share.astype(BF16)
            pre_copy(c).start()

    def prefix(c):
        @pl.when((mb > 0) & (c >= 0) & (c < down_chunks))
        def _():
            pre_copy(c).wait_recv()
            running = run_out[0, run_at(c), :] + pre_r[c].astype(F32).T
            run_out[0, run_at(c), :] = running

            @pl.when(mb < n_mb - 1)
            def _():
                dn[pre_at(c)] = running.T.astype(BF16)
                pre_copy(c).start()

    def lg_step(slot, j):
        total = lg_acc[slot]
        for c in (2 * j, 2 * j + 1):
            total = total + lax.dot_general(
                weight_v[c], grad_v[c, slot], (((1,), (1,)), ((), ())), preferred_element_type=F32)
        lg_acc[slot] = total

    def lg_start(slot):
        lg_send[slot] = lg_acc[slot].astype(BF16)
        for s in others:
            lg_copy(s, slot).start()

    pairs = up_chunks // 2
    lg_acc[...] = jnp.zeros_like(lg_acc)

    @pl.loop(0, LATE)
    def _(i):
        for c in (i, first + i):
            grad_copy(c).wait()
            up_make(0, c)
        up_pass(0, 0, 0, i)

        @pl.when(i > 0)
        def _():
            up_pass(1, 0, 0, first + i - 1)

    @pl.loop(LATE, EARLY)
    def _(c):
        grad_copy(c).wait()
        up_make(0, c)

        @pl.when(c == LATE)
        def _():
            up_pass(1, 0, 0, up_chunks - 1)

    @pl.loop(0, pairs)
    def _(j):
        for c in (2 * j, 2 * j + 1):
            weight_copy(c).wait()

        @pl.when(2 * j == EARLY)
        def _():
            for c in range(EARLY, first):
                grad_copy(c).wait()

        lg_step(0, j)

        @pl.when(j < 2)
        def _():
            up_pass(0, 0, 0, 2 + j)

        @pl.when(j % 2 == 1)
        def _():
            up_pass(0, 1, 0, j // 2)

    lg_start(0)

    @pl.loop(EARLY, first)
    def _(c):
        up_make(0, c)

    up_pass(0, 0, 0, EARLY)
    for s in others:
        lat_copy(s).wait_recv()
        latent_part(s)
        @pl.loop(0, LATE)
        def _(i):
            up_make(s, first + i)

        @pl.loop(0, EARLY)
        def _(c):
            up_make(s, c)

            @pl.when(c < LATE)
            def _():
                up_pass(1, 0, s, first + c)

            @pl.when(c >= 2)
            def _():
                up_pass(0, 0, s, c - 2)

        if s == 1:
            up_pass(0, 1, 0, 2)

    for slot in range(1, slot_count):
        @pl.loop(0, pairs)
        def _(j):
            lg_step(slot, j)
            if slot == 1:
                @pl.when(j < 2)
                def _():
                    for s in others:
                        up_pass(0, 0, s, 2 + j)

                @pl.when(j % 2 == 0)
                def _():
                    up_pass(0, 1, 0, 3 + j // 2)

                @pl.when(j % 2 == 1)
                def _():
                    up_deep(0, 0, j // 2, 2)

        lg_start(slot)

    for c in range(EARLY + 1, first):
        up_pass(0, 0, 0, c)
    up_second(0)
    for s in others:
        @pl.loop(EARLY, first)
        def _(c):
            up_make(s, c)

        for c in range(EARLY, first):
            up_pass(0, 0, s, c)
    up_deep(0, 0, 2, 2)
    up_second(1)
    for c in late:
        for s in range(n_tp):
            up_deep(1, s, c, 1)
        up_copy(1, joints[1], 0, c).start()
    up_second(2)
    up_deep(0, 0, 3, 2)
    up_join(0)
    up_second(3)
    up_join(1)
    up_pass(0, 1, 0, 5)

    for slot in range(slot_count):
        total = lg_acc[slot]
        for s in others:
            lg_copy(s, slot).wait_recv()
            total = total + lg_recv[s - 1, slot].astype(F32)
        token = lax.broadcasted_iota(jnp.int32, total.shape, 1)
        total = jnp.where(token < counts[slot], total, 0.0)
        lg_t[:, slot * cap:(slot + 1) * cap] = total.astype(BF16)

    @pl.loop(0, down_chunks)
    def _(c):
        hidden_copy(c).wait()
        block = lax.dot_general(
            lg_t[...], hidden_v[c % ahead].reshape(rows, down_width),
            (((1,), (0,)), ((), ())), preferred_element_type=F32)
        dn[c] = block.astype(BF16).reshape(dn.shape[1:])
        dn_copy(0, c).start()

        @pl.when(c + ahead < down_chunks)
        def _():
            hidden_copy(c + ahead).start()

        @pl.when(c >= TRAIL)
        def _():
            dn_pass(0, c - TRAIL)

        @pl.when(c == down_chunks * 2 // 7)
        def _():
            up_second(4)
            up_join(2)

        @pl.when(c == down_chunks * 4 // 7)
        def _():
            up_deep(0, 0, 4, 2)
            up_join(3)

        @pl.when(c == down_chunks * 5 // 7)
        def _():
            up_second(5)
            dn_share(0)

        @pl.when(c == down_chunks * 6 // 7)
        def _():
            dn_share(1)

    for c in range(down_chunks - TRAIL, down_chunks):
        dn_pass(0, c)
    for c in late:
        up_pass(1, joints[1], 0, c)

    @pl.loop(2, down_chunks)
    def _(t):
        dn_share(t)

        prefix(t - LAG * mb)

    held = (first - 2, first - 1)
    high = partner[orders[0][joints[0]]][0] == 1

    @pl.loop(0, LAG * (n_mb - 1))
    def _(u):
        @pl.when(high & (u == 2 * mb))
        def _():
            up_deep(0, 0, held[-1], 2)
            for c in held:
                up_join(c)

        prefix(down_chunks + u - LAG * mb)

    @pl.when(jnp.logical_not(high))
    def _():
        up_deep(0, 0, held[-1], 2)
        for c in held:
            for s in others:
                up_deep(0, s, c, 2)
            up_copy(0, joints[0], 0, c).wait_recv()
            up_copy(0, joints[0], 0, c).start()

    @pl.when(high)
    def _():
        for c in held:
            up_copy(0, joints[0], 0, c).wait_recv()

    @pl.loop(0, first - len(held))
    def _(c):
        up_finish(0, c)

    for c in held:
        up_finish(0, c, True)

    for c in late:
        for j in range(joints[1] + 1, last):
            up_pass(1, j, 0, c)
        up_write(1, c)

    for s in others:
        lat_copy(s).wait_send()
        for slot in range(slot_count):
            lg_copy(s, slot).wait_send()

    def up_sent(o, c):
        for k in range(last + 1):
            for s in range(n_tp if k < joints[o] else 1):
                up_copy(o, k, s, c).wait_send()

    @pl.loop(0, first)
    def _(c):
        up_sent(0, c)

    for c in late:
        up_sent(1, c)

    @pl.loop(0, down_chunks)
    def _(c):
        for k in range(n_dp_steps):
            dn_copy(k, c).wait_send()

        @pl.when(mb < n_mb - 1)
        def _():
            pre_copy(c).wait_send()


def local(sizes, hidden, latent, out_grad, up_weight, mb_tokens, slot_mb):
    n_mb, n_tp, n_dp = sizes
    _, slot_count, cap, feature_part = hidden.shape
    rank_part = latent.shape[3]
    rank, column_part = up_weight.shape
    rows = slot_count * cap
    width = column_part // UP_CHUNKS
    down_chunks = next(n for n in (14, 7) if feature_part % (128 * n) == 0)
    down_width = feature_part // down_chunks
    ahead = 2 * down_chunks // 7
    dp_bits, mb_bits = bits_of(n_dp), bits_of(n_mb)
    bits = dp_bits + mb_bits
    up_rows = rank >> bits
    share = rank >> dp_bits
    dma = pltpu.SemaphoreType.DMA
    scratch = [
        pltpu.VMEM((UP_CHUNKS, slot_count, cap, width), BF16),
        pltpu.VMEM((UP_CHUNKS, rank, width), BF16),
        pltpu.VMEM((ahead, slot_count, cap, down_width), BF16),
        pltpu.VMEM((n_tp, slot_count, cap, rank_part), BF16),
        pltpu.VMEM((n_tp, rank_part, rows), BF16),
        pltpu.VMEM((slot_count, rank, cap), F32),
        pltpu.VMEM((slot_count, rank, cap), BF16),
        pltpu.VMEM((n_tp - 1, slot_count, rank, cap), BF16),
        pltpu.VMEM((rank, rows), BF16),
        pltpu.VMEM((UP_CHUNKS,) + (2,) * bits + (up_rows, width), BF16),
        [pltpu.VMEM((UP_CHUNKS,) + (2,) * (bits - 1 - k) + (up_rows, width), BF16) for k in range(bits)],
        pltpu.VMEM((down_chunks,) + (2,) * dp_bits + (share, down_width), BF16),
        [pltpu.VMEM((down_chunks,) + (2,) * (dp_bits - 1 - k) + (share, down_width), BF16) for k in range(dp_bits)],
        pltpu.VMEM((down_chunks, share, down_width), BF16),
        dma((UP_CHUNKS,)), dma((UP_CHUNKS,)), dma((ahead,)), dma,
        dma((n_tp - 1,)), dma((n_tp - 1,)), dma((n_tp - 1, slot_count)), dma((n_tp - 1, slot_count)),
        dma((bits, n_tp, UP_CHUNKS)), dma((bits, n_tp, UP_CHUNKS)),
        dma((dp_bits, down_chunks)), dma((dp_bits, down_chunks)),
        dma((down_chunks,)), dma((down_chunks,)),
    ]
    hbm = pl.BlockSpec(memory_space=pl.ANY)
    smem = pl.BlockSpec(memory_space=pltpu.SMEM)
    vmem = pl.BlockSpec(memory_space=pltpu.VMEM)
    return pl.pallas_call(
        functools.partial(kernel, sizes),
        out_shape=(
            pltpu.VMEM((up_rows, column_part), F32),
            pltpu.VMEM((1, feature_part, share), F32),
        ),
        in_specs=[hbm] * 4 + [smem] * 2,
        out_specs=(vmem, vmem),
        scratch_shapes=scratch,
        compiler_params=pltpu.CompilerParams(
            collective_id=0, has_side_effects=True, vmem_limit_bytes=63700992),
    )(hidden, latent, out_grad, up_weight, mb_tokens, slot_mb)


def solution(mesh):
    sizes = tuple(mesh.shape[axis] for axis in ("mb", "tp", "dp"))
    return jax.shard_map(
        functools.partial(local, sizes),
        mesh=mesh,
        in_specs=(
            P("dp", "mb", None, "tp"),
            P("dp", "mb", None, "tp"),
            P("dp", "mb", None, "tp"),
            P(None, "tp"),
            P("dp", None),
            P("dp", "mb"),
        ),
        out_specs=(P(("mb", "dp"), "tp"), P("mb", "tp", "dp")),
        check_vma=False,
    )
```

```python
import functools

import jax
import jax.numpy as jnp
from jax import lax
from jax.experimental import pallas as pl
from jax.experimental.pallas import tpu as pltpu
from jax.sharding import PartitionSpec as P

F32 = jnp.float32
BF16 = jnp.bfloat16
UP_CHUNKS = 8
LATE = 2
EARLY = 4
LAG = 4
TRAIL = 2
SENT = 8


def bits_of(size):
    count = size.bit_length() - 1
    assert size == 1 << count, "axis size"
    return count


def kernel(sizes, hidden, latent, grad, weight, tokens, slots, up_out, run_out,
           grad_v, weight_v, hidden_v, lat_v, lat_t, lg_acc, lg_send, lg_recv, lg_t,
           up, up_r, dn, dn_r, pre_r,
           grad_sem, weight_sem, hidden_sem, lat_sem, lat_ss, lat_rs, lg_ss, lg_rs,
           up_ss, up_rs, dn_ss, dn_rs, pre_ss, pre_rs):
    n_mb, n_tp, n_dp = sizes
    mb, tp, dp = (lax.axis_index(a) for a in ("mb", "tp", "dp"))
    up_chunks, slot_count, cap, width = grad_v.shape
    rows = slot_count * cap
    rank_part = lat_v.shape[-1]
    down_chunks, down_width = dn.shape[0], dn.shape[-1]
    ahead = hidden_v.shape[0]

    dims, partner = [], {}
    for axis, index, size in (("mb", mb, n_mb), ("dp", dp, n_dp)):
        for k in reversed(range(bits_of(size))):
            bit = (index // (1 << k)) % 2
            dims.append((axis, k))
            partner[axis, k] = bit, {axis: index + (1 - 2 * bit) * (1 << k)}
    tp_bits, n_dp_steps = bits_of(n_tp), bits_of(n_dp)
    part_dims = dims[:tp_bits]
    last = len(dims) - 1
    dp_first = dims[::-1]
    mb_first = dp_first[:1] + dp_first[n_dp_steps:] + dp_first[1:n_dp_steps]
    orders = (dp_first, mb_first)
    joints = [min(order.index(d) for d in part_dims) if part_dims else last for order in orders]
    tp_peers = [{"tp": (tp + s) % n_tp} for s in range(1, n_tp)]
    following, preceding = {"mb": (mb + 1) % n_mb}, {"mb": (mb + n_mb - 1) % n_mb}

    def grad_copy(c):
        return pltpu.make_async_copy(
            grad.at[0, :, :, pl.ds(pl.multiple_of(c * width, width), width)], grad_v.at[c], grad_sem.at[c])

    def weight_copy(c):
        return pltpu.make_async_copy(
            weight.at[:, pl.ds(pl.multiple_of(c * width, width), width)], weight_v.at[c], weight_sem.at[c])

    def hidden_copy(c):
        return pltpu.make_async_copy(
            hidden.at[0, :, :, pl.ds(pl.multiple_of(c * down_width, down_width), down_width)],
            hidden_v.at[c % ahead], hidden_sem.at[c % ahead])

    def remote(src, dst, ss, rs, to):
        return pltpu.make_async_remote_copy(
            src_ref=src, dst_ref=dst, send_sem=ss, recv_sem=rs,
            device_id=to, device_id_type=pl.DeviceIdType.MESH)

    barrier = pltpu.get_barrier_semaphore()
    greeted = [to for _, to in partner.values()] + tp_peers + [following, preceding]
    for to in greeted:
        pl.semaphore_signal(barrier, inc=1, device_id=to, device_id_type=pl.DeviceIdType.MESH)

    own_latent = pltpu.make_async_copy(latent.at[0], lat_v.at[0], lat_sem)
    own_latent.start()
    first = up_chunks - LATE
    late = range(first, up_chunks)
    fetched = [c for i in range(LATE) for c in (first + i, i)] + list(range(LATE, first))
    grad_copy(fetched[0]).start()

    counts = [tokens[0, slots[0, s]] for s in range(slot_count)]

    def live(shape):
        row = lax.broadcasted_iota(jnp.int32, shape, 0)
        valid = row < counts[0]
        for s in range(1, slot_count):
            valid = valid | ((row >= s * cap) & (row < s * cap + counts[s]))
        return valid

    def latent_part(s):
        part = lat_v[s].reshape(rows, rank_part).astype(F32)
        part = jnp.where(live(part.shape), part, 0.0)
        lat_t[s] = part.T.astype(BF16)

    own_latent.wait()
    for c in fetched[1:3]:
        grad_copy(c).start()
    latent_part(0)
    pl.semaphore_wait(barrier, len(greeted))

    def lat_copy(s):
        return remote(lat_v.at[0], lat_v.at[s], lat_ss.at[s - 1], lat_rs.at[s - 1], tp_peers[s - 1])

    def lg_copy(s, slot):
        return remote(lg_send.at[slot], lg_recv.at[s - 1, slot],
                      lg_ss.at[s - 1, slot], lg_rs.at[s - 1, slot], tp_peers[s - 1])

    for s in range(1, n_tp):
        lat_copy(s).start()
    for c in fetched[3:]:
        grad_copy(c).start()
    for c in range(up_chunks):
        weight_copy(c).start()
    for c in range(ahead):
        hidden_copy(c).start()

    def part_at(s):
        part = (tp + n_tp - s) % n_tp
        return {d: (part // (1 << k)) % 2 for k, d in enumerate(reversed(part_dims))}

    def up_refs(o, k, s, c, side):
        step = orders[o][k]
        bit, to = partner[step]
        fixed = part_at(s) if k < joints[o] else {}
        taken = {**fixed, step: (1 - bit) if side else bit}
        before = [d for d in dims if d not in orders[o][:k]]
        after = [d for d in before if d != step]
        src = (up if k == 0 else up_r[k - 1], (c,) + tuple(taken.get(d, slice(None)) for d in before))
        dst = (up_r[k], (c,) + tuple(fixed.get(d, slice(None)) for d in after))
        return src, dst, to

    def up_copy(o, k, s, c):
        (src, at), (dst, to_at), to = up_refs(o, k, s, c, 1)
        return remote(src.at[at], dst.at[to_at], up_ss.at[k, s, c], up_rs.at[k, s, c], to)

    def up_add(o, k, s, c, waited=False):
        (src, at), (dst, to_at), _ = up_refs(o, k, s, c, 0)
        if not waited:
            up_copy(o, k, s, c).wait_recv()
        return src[at].astype(F32) + dst[to_at].astype(F32)

    def up_pass(o, k, s, c, waited=False):
        _, (dst, to_at), _ = up_refs(o, k, s, c, 0)
        dst[to_at] = up_add(o, k, s, c, waited).astype(BF16)
        if k + 1 != joints[o]:
            up_copy(o, k + 1, s, c).start()

    def up_make(s, c):
        block = lax.dot_general(
            lat_t[s], grad_v[c].reshape(rows, width),
            (((1,), (0,)), ((), ())), preferred_element_type=F32).astype(BF16)
        fixed = part_at(s)
        head = tuple(fixed[d] for d in part_dims)
        up[(c,) + head] = block.reshape(up.shape[1 + tp_bits:])
        up_copy(0, 0, s, c).start()

    def up_deep(o, s, c, k):
        for j in range(k, joints[o]):
            up_pass(o, j, s, c)

    def up_finish(o, c, waited=False):
        for j in range(joints[o], last):
            up_pass(o, j, 0, c, waited and j == joints[o])
        up_write(o, c, waited and joints[o] == last)

    def up_write(o, c, waited=False):
        at = pl.ds(pl.multiple_of(c * width, width), width)
        up_out[:, at] = up_add(o, last, 0, c, waited)

    others = range(1, n_tp)

    def up_second(c):
        for s in others:
            up_pass(0, 1, s, c)

    def up_join(c):
        for s in others:
            up_deep(0, s, c, 2)
        up_copy(0, joints[0], 0, c).start()

    def dn_copy(k, c):
        bit, to = partner["dp", k]
        src = (dn if k == 0 else dn_r[k - 1]).at[c]
        index = (slice(None),) * (n_dp_steps - 1 - k) + (1 - bit,)
        return remote(src.at[index], dn_r[k].at[c], dn_ss.at[k, c], dn_rs.at[k, c], to)

    def dn_add(k, c):
        bit, _ = partner["dp", k]
        dn_copy(k, c).wait_recv()
        src = dn if k == 0 else dn_r[k - 1]
        kept = src[(c,) + (slice(None),) * (n_dp_steps - 1 - k) + (bit,)]
        return kept.astype(F32) + dn_r[k][c].astype(F32)

    def dn_pass(k, c):
        dn_r[k][c] = dn_add(k, c).astype(BF16)
        dn_copy(k + 1, c).start()

    halves = pre_ss.shape[1]
    half = down_width // halves

    def pre_copy(c, h):
        at = slice(None), pl.ds(h * half, half)
        return remote(dn.at[pre_at(c) + at], pre_r.at[(c,) + at], pre_ss.at[c, h], pre_rs.at[c, h], following)

    def pre_sent(c):
        for h in range(halves):
            pre_copy(c, h).wait_send()

    def pre_at(c):
        return (c,) + (0,) * (n_dp_steps - 1) + (partner["dp", 0][0],)

    def run_at(c):
        return pl.ds(pl.multiple_of(c * down_width, down_width), down_width)

    def dn_share(c):
        for k in range(1, n_dp_steps - 1):
            dn_pass(k, c)
        share = dn_add(n_dp_steps - 1, c)

        run_out[0, run_at(c), :] = share.T

        @pl.when(mb == 0)
        def _():
            dn[pre_at(c)] = share.astype(BF16)
            for h in range(halves):
                pre_copy(c, h).start()

    def prefix(c):
        @pl.when((mb < n_mb - 1) & (c >= SENT) & (c < down_chunks + SENT))
        def _():
            pre_sent(c - SENT)

        @pl.when((mb > 0) & (c >= 0) & (c < down_chunks))
        def _():
            for h in range(halves):
                cols = pl.ds(h * half, half)
                rows_at = pl.ds(pl.multiple_of(c * down_width + h * half, half), half)
                pre_copy(c, h).wait_recv()
                running = run_out[0, rows_at, :] + pre_r[c, :, cols].astype(F32).T
                run_out[0, rows_at, :] = running

                @pl.when(mb < n_mb - 1)
                def _():
                    dn[pre_at(c) + (slice(None), cols)] = running.T.astype(BF16)
                    pre_copy(c, h).start()

    def lg_step(slot, j):
        total = lg_acc[slot]
        for c in (2 * j, 2 * j + 1):
            total = total + lax.dot_general(
                weight_v[c], grad_v[c, slot], (((1,), (1,)), ((), ())), preferred_element_type=F32)
        lg_acc[slot] = total

    def lg_start(slot):
        lg_send[slot] = lg_acc[slot].astype(BF16)
        for s in others:
            lg_copy(s, slot).start()

    pairs = up_chunks // 2
    lg_acc[...] = jnp.zeros_like(lg_acc)

    @pl.loop(0, LATE)
    def _(i):
        grad_copy(first + i).wait()
        up_make(0, first + i)

        @pl.when(i > 0)
        def _():
            up_pass(0, 0, 0, i - 1)

        grad_copy(i).wait()
        up_make(0, i)
        up_pass(1, 0, 0, first + i)

    @pl.loop(LATE, EARLY)
    def _(c):
        grad_copy(c).wait()
        up_make(0, c)

        @pl.when(c == LATE)
        def _():
            up_pass(0, 0, 0, LATE - 1)

    @pl.loop(0, pairs)
    def _(j):
        for c in (2 * j, 2 * j + 1):
            weight_copy(c).wait()

        @pl.when(2 * j == EARLY)
        def _():
            for c in range(EARLY, first):
                grad_copy(c).wait()

        lg_step(0, j)

        @pl.when(j < 2)
        def _():
            up_pass(0, 0, 0, 2 + j)

        @pl.when(j % 2 == 1)
        def _():
            up_pass(0, 1, 0, j // 2)

    lg_start(0)

    @pl.loop(EARLY, first)
    def _(c):
        up_make(0, c)

    up_pass(0, 0, 0, EARLY)
    for s in others:
        lat_copy(s).wait_recv()
        latent_part(s)
        @pl.loop(0, LATE)
        def _(i):
            up_make(s, first + i)

        if s == 1:
            up_pass(0, 1, 0, 2)

        @pl.loop(0, EARLY)
        def _(c):
            up_make(s, c)

            @pl.when(c < LATE)
            def _():
                up_pass(1, 0, s, first + c)

            @pl.when(c >= 2)
            def _():
                up_pass(0, 0, s, c - 2)

        if s == 1:
            up_pass(0, 1, 0, 3)

    for slot in range(1, slot_count):
        @pl.loop(0, pairs)
        def _(j):
            lg_step(slot, j)
            if slot == 1:
                @pl.when(j < 2)
                def _():
                    for s in others:
                        up_pass(0, 0, s, 2 + j)

                @pl.when(j == 2)
                def _():
                    up_pass(0, 1, 0, 4)

                @pl.when(j % 2 == 1)
                def _():
                    up_deep(0, 0, j // 2, 2)

        lg_start(slot)

    for c in range(EARLY + 1, first):
        up_pass(0, 0, 0, c)
    up_second(0)
    for s in others:
        @pl.loop(EARLY, first)
        def _(c):
            up_make(s, c)

        for c in range(EARLY, first):
            up_pass(0, 0, s, c)
    up_deep(0, 0, 2, 2)
    up_second(1)
    for c in late:
        for s in range(n_tp):
            up_deep(1, s, c, 1)
        up_copy(1, joints[1], 0, c).start()
    up_second(2)
    up_deep(0, 0, 3, 2)
    up_join(0)
    up_second(3)
    up_join(1)
    up_pass(0, 1, 0, 5)

    for slot in range(slot_count):
        total = lg_acc[slot]
        for s in others:
            lg_copy(s, slot).wait_recv()
            total = total + lg_recv[s - 1, slot].astype(F32)
        token = lax.broadcasted_iota(jnp.int32, total.shape, 1)
        total = jnp.where(token < counts[slot], total, 0.0)
        lg_t[:, slot * cap:(slot + 1) * cap] = total.astype(BF16)

    @pl.loop(0, down_chunks)
    def _(c):
        hidden_copy(c).wait()
        block = lax.dot_general(
            lg_t[...], hidden_v[c % ahead].reshape(rows, down_width),
            (((1,), (0,)), ((), ())), preferred_element_type=F32)
        dn[c] = block.astype(BF16).reshape(dn.shape[1:])
        dn_copy(0, c).start()

        @pl.when(c + ahead < down_chunks)
        def _():
            hidden_copy(c + ahead).start()

        @pl.when(c >= TRAIL)
        def _():
            dn_pass(0, c - TRAIL)

        @pl.when(c == down_chunks * 2 // 7)
        def _():
            up_second(4)
            up_join(2)

        @pl.when(c == down_chunks * 4 // 7)
        def _():
            up_deep(0, 0, 4, 2)
            up_join(3)

        @pl.when(c == down_chunks * 5 // 7)
        def _():
            up_second(5)
            dn_share(0)

        @pl.when(c == down_chunks * 6 // 7)
        def _():
            dn_share(1)

    for c in range(down_chunks - TRAIL, down_chunks):
        dn_pass(0, c)
    for c in late:
        up_pass(1, joints[1], 0, c)

    held = (first - 2, first - 1)
    axis_bit = orders[0][joints[0]]
    upper = partner[axis_bit][0]
    high = upper == 1
    holds = mb == upper * (1 << axis_bit[1])

    def join_held():
        up_deep(0, 0, held[-1], 2)
        for c in held:
            up_join(c)

    settled = max(0, min(first, down_chunks - SENT))

    def up_sent(o, c, steps):
        for k in steps:
            for s in range(n_tp if k < joints[o] else 1):
                up_copy(o, k, s, c).wait_send()

    @pl.loop(2, down_chunks)
    def _(t):
        dn_share(t)

        @pl.when((t == 4) & jnp.logical_not(holds))
        def _():
            join_held()

        prefix(t - LAG * mb)
        dn_copy(0, t).wait_send()
        for k in range(1, n_dp_steps):
            dn_copy(k, t - 2).wait_send()

        @pl.when(t == 5)
        def _():
            for s in others:
                lat_copy(s).wait_send()
                for slot in range(slot_count):
                    lg_copy(s, slot).wait_send()
            for c in late:
                up_sent(1, c, range(joints[1]))

        @pl.when((t >= SENT) & (t < SENT + settled))
        def _():
            up_sent(0, t - SENT, range(joints[0]))

    @pl.loop(0, LAG * (n_mb - 1))
    def _(u):
        @pl.when(holds & high & (u == 2))
        def _():
            join_held()

        prefix(down_chunks + u - LAG * mb)

    @pl.when(holds & jnp.logical_not(high))
    def _():
        up_deep(0, 0, held[-1], 2)
        for c in held:
            for s in others:
                up_deep(0, s, c, 2)
            up_copy(0, joints[0], 0, c).wait_recv()
            up_copy(0, joints[0], 0, c).start()

    @pl.when(high | jnp.logical_not(holds))
    def _():
        for c in held:
            up_copy(0, joints[0], 0, c).wait_recv()

    @pl.loop(0, first - len(held))
    def _(c):
        up_finish(0, c)

    for c in held:
        up_finish(0, c, True)

    for c in late:
        for j in range(joints[1] + 1, last):
            up_pass(1, j, 0, c)
        up_write(1, c)

    for c in range(settled, first):
        up_sent(0, c, range(joints[0]))

    @pl.loop(0, first)
    def _(c):
        up_sent(0, c, range(joints[0], last + 1))

    for c in late:
        up_sent(1, c, range(joints[1], last + 1))

    for c in range(2):
        dn_copy(0, c).wait_send()
        for k in range(1, n_dp_steps):
            dn_copy(k, down_chunks - 1 - c).wait_send()

    waited = down_chunks + LAG * (n_mb - 1) - LAG * mb - SENT

    @pl.loop(0, down_chunks)
    def _(c):
        @pl.when((mb < n_mb - 1) & (c >= waited))
        def _():
            pre_sent(c)


def local(sizes, hidden, latent, out_grad, up_weight, mb_tokens, slot_mb):
    n_mb, n_tp, n_dp = sizes
    _, slot_count, cap, feature_part = hidden.shape
    rank_part = latent.shape[3]
    rank, column_part = up_weight.shape
    rows = slot_count * cap
    width = column_part // UP_CHUNKS
    down_chunks = next(n for n in (14, 7) if feature_part % (128 * n) == 0)
    down_width = feature_part // down_chunks
    ahead = 2 * down_chunks // 7
    halves = 2 if down_width % 256 == 0 else 1
    dp_bits, mb_bits = bits_of(n_dp), bits_of(n_mb)
    bits = dp_bits + mb_bits
    up_rows = rank >> bits
    share = rank >> dp_bits
    dma = pltpu.SemaphoreType.DMA
    scratch = [
        pltpu.VMEM((UP_CHUNKS, slot_count, cap, width), BF16),
        pltpu.VMEM((UP_CHUNKS, rank, width), BF16),
        pltpu.VMEM((ahead, slot_count, cap, down_width), BF16),
        pltpu.VMEM((n_tp, slot_count, cap, rank_part), BF16),
        pltpu.VMEM((n_tp, rank_part, rows), BF16),
        pltpu.VMEM((slot_count, rank, cap), F32),
        pltpu.VMEM((slot_count, rank, cap), BF16),
        pltpu.VMEM((n_tp - 1, slot_count, rank, cap), BF16),
        pltpu.VMEM((rank, rows), BF16),
        pltpu.VMEM((UP_CHUNKS,) + (2,) * bits + (up_rows, width), BF16),
        [pltpu.VMEM((UP_CHUNKS,) + (2,) * (bits - 1 - k) + (up_rows, width), BF16) for k in range(bits)],
        pltpu.VMEM((down_chunks,) + (2,) * dp_bits + (share, down_width), BF16),
        [pltpu.VMEM((down_chunks,) + (2,) * (dp_bits - 1 - k) + (share, down_width), BF16) for k in range(dp_bits)],
        pltpu.VMEM((down_chunks, share, down_width), BF16),
        dma((UP_CHUNKS,)), dma((UP_CHUNKS,)), dma((ahead,)), dma,
        dma((n_tp - 1,)), dma((n_tp - 1,)), dma((n_tp - 1, slot_count)), dma((n_tp - 1, slot_count)),
        dma((bits, n_tp, UP_CHUNKS)), dma((bits, n_tp, UP_CHUNKS)),
        dma((dp_bits, down_chunks)), dma((dp_bits, down_chunks)),
        dma((down_chunks, halves)), dma((down_chunks, halves)),
    ]
    hbm = pl.BlockSpec(memory_space=pl.ANY)
    smem = pl.BlockSpec(memory_space=pltpu.SMEM)
    vmem = pl.BlockSpec(memory_space=pltpu.VMEM)
    return pl.pallas_call(
        functools.partial(kernel, sizes),
        out_shape=(
            pltpu.VMEM((up_rows, column_part), F32),
            pltpu.VMEM((1, feature_part, share), F32),
        ),
        in_specs=[hbm] * 4 + [smem] * 2,
        out_specs=(vmem, vmem),
        scratch_shapes=scratch,
        compiler_params=pltpu.CompilerParams(
            collective_id=0, has_side_effects=True, vmem_limit_bytes=63700992),
    )(hidden, latent, out_grad, up_weight, mb_tokens, slot_mb)


def solution(mesh):
    sizes = tuple(mesh.shape[axis] for axis in ("mb", "tp", "dp"))
    return jax.shard_map(
        functools.partial(local, sizes),
        mesh=mesh,
        in_specs=(
            P("dp", "mb", None, "tp"),
            P("dp", "mb", None, "tp"),
            P("dp", "mb", None, "tp"),
            P(None, "tp"),
            P("dp", None),
            P("dp", "mb"),
        ),
        out_specs=(P(("mb", "dp"), "tp"), P("mb", "tp", "dp")),
        check_vma=False,
    )
```
